32 devices in a mesh: rep: 1, dp: 32 (over x, y, z, core).
Axes of the slice: x: 2, y: 2, z: 4, core: 2. Of those that a mesh axis runs over, the one named last changes fastest.
Arguments:
- g_w_gate: bfloat16 [32, 2, 1024, 3072], P(('rep', 'dp'))
- g_w_up: bfloat16 [32, 2, 1024, 3072], P(('rep', 'dp'))
- g_w_down: bfloat16 [32, 2, 3072, 1024], P(('rep', 'dp'))
- w_gate: bfloat16 [2, 1024, 3072], replicated
- w_up: bfloat16 [2, 1024, 3072], replicated
- w_down: bfloat16 [2, 3072, 1024], replicated
- m_w_gate: float32 [2, 1024, 3072], P(None, 'dp')
- m_w_up: float32 [2, 1024, 3072], P(None, 'dp')
- m_w_down: float32 [2, 3072, 1024], P(None, 'dp')
- v_w_gate: float32 [2, 1024, 3072], P(None, 'dp')
- v_w_up: float32 [2, 1024, 3072], P(None, 'dp')
- v_w_down: float32 [2, 3072, 1024], P(None, 'dp')
Outputs:
- output 1: bfloat16 [2, 1024, 3072], P('rep')
- output 2: bfloat16 [2, 1024, 3072], P('rep')
- output 3: bfloat16 [2, 3072, 1024], P('rep')
- output 4: float32 [2, 1024, 3072], P('rep', 'dp')
- output 5: float32 [2, 1024, 3072], P('rep', 'dp')
- output 6: float32 [2, 3072, 1024], P('rep', 'dp')
- output 7: float32 [2, 1024, 3072], P('rep', 'dp')
- output 8: float32 [2, 1024, 3072], P('rep', 'dp')
- output 9: float32 [2, 3072, 1024], P('rep', 'dp')
All inputs are finite; a program needn't handle non-finite values.
Results may differ from the reference program's by a relative error of at most 0.022.
Values are sent between devices in bfloat16 or wider.
A program may use at most 2 GiB of HBM per device.

```python
import jax
import jax.numpy as jnp
from jax import lax

DEVICES = 32
D = 1024
FF = 3072
LAYERS = 2
NAMES = ("w_gate", "w_up", "w_down")
SHAPES = {"w_gate": (LAYERS, D, FF), "w_up": (LAYERS, D, FF), "w_down": (LAYERS, FF, D)}


def setup_inputs(seed: int = 0, part: int = 0) -> dict:
    kz, *keys = jax.random.split(jax.random.key(seed), 1 + 5 * len(NAMES))
    loud = 2.0 ** jax.random.uniform(kz, (), jnp.float32, -1.0, 1.0)
    drawn = {}
    for name, key, both in zip(NAMES, keys[:3], keys[3:6], strict=True):
        own = jax.random.normal(jax.random.fold_in(key, part), (DEVICES, *SHAPES[name]), jnp.float32)
        shared = jax.random.normal(jax.random.fold_in(both, part), SHAPES[name], jnp.float32)
        drawn["g_" + name] = (loud * (0.7 * shared / DEVICES + 0.7 * own * DEVICES**-0.5)).astype(jnp.bfloat16)
    for name, key in zip(NAMES, keys[6:9], strict=True):
        drawn[name] = (jax.random.normal(key, SHAPES[name], jnp.float32) * SHAPES[name][1] ** -0.5).astype(jnp.bfloat16)
    for name, key in zip(NAMES, keys[9:12], strict=True):
        drawn["m_" + name] = loud * 0.5 * jax.random.normal(key, SHAPES[name], jnp.float32)
    for name, key in zip(NAMES, keys[12:15], strict=True):
        drawn["v_" + name] = loud * loud * jax.random.uniform(key, SHAPES[name], jnp.float32, 0.5, 1.5)
    return drawn


def adamw(w, m, v, g):
    m = 0.9 * m + 0.1 * g
    v = 0.95 * v + 0.05 * g * g
    step = m * lax.rsqrt(v + 1e-8) + 0.1 * w
    return (w - 0.02 * step).astype(jnp.bfloat16), m, v


def reference(g_w_gate, g_w_up, g_w_down, w_gate, w_up, w_down, m_w_gate, m_w_up, m_w_down, v_w_gate, v_w_up, v_w_down):
    def total(terms):
        return lax.scan(lambda so_far, term: (so_far + term.astype(jnp.float32), None), jnp.zeros(terms.shape[1:], jnp.float32), terms)[0]

    gradients = [total(terms).astype(jnp.bfloat16).astype(jnp.float32) for terms in (g_w_gate, g_w_up, g_w_down)]
    new = [
        adamw(w.astype(jnp.float32), m, v, g)
        for w, m, v, g in zip((w_gate, w_up, w_down), (m_w_gate, m_w_up, m_w_down), (v_w_gate, v_w_up, v_w_down), gradients, strict=True)
    ]
    return tuple(one[which] for which in range(3) for one in new)
```

```python
import jax
import jax.numpy as jnp
from jax import lax
from jax.experimental import pallas as pl
from jax.experimental.pallas import tpu as pltpu
from jax.sharding import PartitionSpec as P

MESH = pl.DeviceIdType.MESH
STRIDE = {"x": 16, "y": 8, "h": 4, "l": 2, "c": 1}
DIMS = "xyhl"
ROWS, COLS = 32, 1024
PER_MATRIX = 6
UNITS = 18
ORDERS = ("xyhl", "yxhl", "lxyh", "xylh", "yxlh", "lyxh", "xyhl", "yxhl", "lxyh", "xylh", "yxlh", "lyxh", "xyhl", "yxhl", "lxyh", "xylh", "yxlh", "lyxh")
EVENTS = (
    0, 11, 22, 33, 44, 1, 55, 12, 66, 23, 77, 34, 88, 45, 99, 56, 110, 121, 132, 143, 154, 165, 67, 176, 78, 187, 89, 13, 2, 122,
    24, 35, 46, 57, 155, 100, 68, 111, 3, 188, 79, 90, 25, 123, 14, 58, 36, 133, 144, 47, 69, 4, 80, 112, 101, 26, 156, 91, 37,
    15, 177, 48, 124, 59, 5, 166, 70, 134, 16, 81, 113, 102, 27, 6, 145, 189, 71, 92, 82, 17, 157, 38, 178, 49, 28, 60, 167, 72,
    7, 190, 83, 18, 179, 29, 93, 39, 103, 50, 168, 114, 61, 19, 40, 125, 8, 135, 73, 30, 51, 62, 146, 84, 20, 94, 158, 21, 104, 9,
    41, 115, 10, 126, 52, 31, 74, 169, 136, 32, 180, 85, 63, 191, 147, 159, 95, 137, 105, 116, 42, 127, 43, 53, 170, 54, 64, 181,
    65, 148, 192, 75, 138, 160, 76, 86, 106, 96, 87, 117, 161, 128, 171, 149, 107, 118, 182, 193, 129, 139, 97, 98, 172, 162, 119,
    108, 120, 109, 194, 183, 140, 150, 184, 173, 130, 195, 131, 141, 142, 163, 185, 164, 151, 186, 196, 197, 174, 175, 152, 153,
)


def adamw(w, m, v, g):
    m = 0.9 * m + 0.1 * g
    v = 0.95 * v + 0.05 * g * g
    step = m * lax.rsqrt(v + 1e-8) + 0.1 * w
    return (w - 0.02 * step).astype(jnp.bfloat16), m, v


def kernel(*refs):
    g_in, w_in, m_in, v_in, w_out, m_out, v_out = (refs[i : i + 3] for i in range(0, 21, 3))
    own, rx0, rx1, rx2, rx3, rx4, w_buf, m_buf, v_buf, w_new, rs_send, rs_recv, ag_send, ag_recv, local = refs[21:]
    rx = (rx0, rx1, rx2, rx3, rx4)
    me = lax.axis_index("dp")
    bit = {d: (me // s) % 2 for d, s in STRIDE.items()}
    partner = {d: me + (1 - 2 * bit[d]) * s for d, s in STRIDE.items()}
    every = slice(None)

    barrier = pltpu.get_barrier_semaphore()
    for d in STRIDE:
        pl.semaphore_signal(barrier, inc=1, device_id=(0, partner[d]), device_id_type=MESH)
    pl.semaphore_wait(barrier, len(STRIDE))

    def place(u):
        which, rest = divmod(u, PER_MATRIX)
        layer, part = divmod(rest, PER_MATRIX // 2)
        if which < 2:
            return which, layer, (every, pl.ds(part * COLS, COLS))
        return which, layer, (pl.ds(part * ROWS, ROWS), every)

    def blocks(ref, u, at, core):
        _, layer, within = place(u)
        return ref.at[(layer, *(at.get(d, every) for d in DIMS), core, *within)]

    def mine(ref, u):
        _, layer, within = place(u)
        return ref.at[(layer, *within)]

    def fixed(u, k, flip):
        at = {d: bit[d] for d in ORDERS[u][:k]}
        if flip:
            at[ORDERS[u][k - 1]] = 1 - bit[ORDERS[u][k - 1]]
        return at

    def remote(src, dst, send, recv, d):
        return pltpu.make_async_remote_copy(
            src_ref=src, dst_ref=dst, send_sem=send, recv_sem=recv, device_id=(0, partner[d]), device_id_type=MESH
        )

    def scatter(u, k):
        if k == 0:
            src, d = blocks(g_in[place(u)[0]], u, {}, 1 - bit["c"]), "c"
        else:
            at, d = fixed(u, k, True), ORDERS[u][k - 1]
            src = own.at[(u, *(at.get(d, every) for d in DIMS))]
        return remote(src, rx[k].at[u], rs_send.at[u, k], rs_recv.at[u, k], d)

    def gather(u, k, receive=False):
        ref, at, core = w_out[place(u)[0]], fixed(u, k, receive and k > 0), bit["c"]
        if k == 0 and receive:
            core = 1 - core
        dst = blocks(ref, u, at, core)
        src = w_new.at[u] if k == 4 else dst
        return remote(src, dst, ag_send.at[u, k], ag_recv.at[u, k], ORDERS[u][k - 1] if k else "c")

    def copy(src, dst, u, i):
        return pltpu.make_async_copy(src, dst, local.at[u, i])

    def load_own(u):
        return copy(blocks(g_in[place(u)[0]], u, {}, bit["c"]), own.at[u], u, 0)

    def loads(u):
        which = place(u)[0]
        return (
            copy(blocks(w_in[which], u, bit, bit["c"]), w_buf.at[u], u, 1),
            copy(mine(m_in[which], u), m_buf.at[u], u, 2),
            copy(mine(v_in[which], u), v_buf.at[u], u, 3),
        )

    def stores(u):
        which = place(u)[0]
        return (
            copy(w_new.at[u], blocks(w_out[which], u, bit, bit["c"]), u, 4),
            copy(m_buf.at[u], mine(m_out[which], u), u, 5),
            copy(v_buf.at[u], mine(v_out[which], u), u, 6),
        )

    def total(u, at, steps, rows):
        so_far = own[(u, *(at[d] for d in DIMS), rows)].astype(jnp.float32)
        for j in range(steps):
            left = [d for d in DIMS if d not in ORDERS[u][:j]]
            so_far += rx[j][(u, *(at[d] for d in left), rows)].astype(jnp.float32)
        return so_far

    def reduce_to_send(u, k):
        base = fixed(u, k, True)
        free = [d for d in DIMS if d not in base]

        def body(i, carry):
            at = dict(base)
            for p, d in enumerate(reversed(free)):
                at[d] = (i // 2**p) % 2
            for half in range(2):
                rows = pl.ds(half * (ROWS // 2), ROWS // 2)
                own[(u, *(at[d] for d in DIMS), rows)] = total(u, at, k, rows).astype(jnp.bfloat16)
            return carry

        lax.fori_loop(0, 2 ** len(free), body, 0)

    def update(u):
        for half in range(2):
            rows = pl.ds(half * (ROWS // 2), ROWS // 2)
            g = total(u, bit, 5, rows).astype(jnp.bfloat16).astype(jnp.float32)
            w_new[u, rows], m_buf[u, rows], v_buf[u, rows] = adamw(w_buf[u, rows].astype(jnp.float32), m_buf[u, rows], v_buf[u, rows], g)

    def event(u, e):
        if e == 0:
            scatter(u, 0).start()
            load_own(u).start()
        elif e <= 4:
            if e == 1:
                load_own(u).wait()
                for one in loads(u):
                    one.start()
            scatter(u, e - 1).wait_recv()
            reduce_to_send(u, e)
            scatter(u, e).start()
        elif e == 5:
            for one in loads(u):
                one.wait()
            scatter(u, 4).wait_recv()
            update(u)
            gather(u, 4).start()
            for one in stores(u):
                one.start()
        elif e <= 9:
            if e == 6:
                for one in stores(u):
                    one.wait()
            gather(u, 10 - e, receive=True).wait_recv()
            gather(u, 9 - e).start()
        else:
            gather(u, 0, receive=True).wait_recv()

    for code in EVENTS:
        event(*divmod(code, 11))
    for u in range(UNITS):
        for k in range(5):
            scatter(u, k).wait_send()
            gather(u, k).wait_send()


def solution(mesh):
    def step(*arrays):
        split = [(2, 2, 2, 2, 2, 2, a.shape[-2] // 32, a.shape[-1]) for a in arrays[:3]]
        terms = [a.reshape(s) for a, s in zip(arrays[:3], split)]
        weights = [a.reshape(s) for a, s in zip(arrays[3:6], split)]
        block = (UNITS, ROWS, COLS)
        dma = pltpu.SemaphoreType.DMA
        anywhere = pl.BlockSpec(memory_space=pl.ANY)
        out = pl.pallas_call(
            kernel,
            out_shape=[jax.ShapeDtypeStruct(s, jnp.bfloat16) for s in split] + [jax.ShapeDtypeStruct(a.shape, a.dtype) for a in arrays[6:]],
            in_specs=[anywhere] * 12,
            out_specs=[anywhere] * 9,
            scratch_shapes=[
                pltpu.VMEM((UNITS, 2, 2, 2, 2, ROWS, COLS), jnp.bfloat16),
                pltpu.VMEM((UNITS, 2, 2, 2, 2, ROWS, COLS), jnp.bfloat16),
                pltpu.VMEM((UNITS, 2, 2, 2, ROWS, COLS), jnp.bfloat16),
                pltpu.VMEM((UNITS, 2, 2, ROWS, COLS), jnp.bfloat16),
                pltpu.VMEM((UNITS, 2, ROWS, COLS), jnp.bfloat16),
                pltpu.VMEM(block, jnp.bfloat16),
                pltpu.VMEM(block, jnp.bfloat16),
                pltpu.VMEM(block, jnp.float32),
                pltpu.VMEM(block, jnp.float32),
                pltpu.VMEM(block, jnp.bfloat16),
                dma((UNITS, 5)),
                dma((UNITS, 5)),
                dma((UNITS, 5)),
                dma((UNITS, 5)),
                dma((UNITS, 7)),
            ],
            compiler_params=pltpu.CompilerParams(collective_id=0, has_side_effects=True, vmem_limit_bytes=67_043_328),
            name="zero_step",
        )(*terms, *weights, *arrays[6:])
        return (*(o.reshape(a.shape) for o, a in zip(out[:3], arrays[3:6])), *out[3:])

    all_of, cut = P(None, None, None), P(None, "dp", None)
    return jax.shard_map(
        step,
        mesh=mesh,
        in_specs=(P(("rep", "dp"), None, None, None),) * 3 + (all_of,) * 3 + (cut,) * 6,
        out_specs=(P("rep", None, None),) * 3 + (P("rep", "dp", None),) * 6,
        check_vma=False,
    )
```

```python
import jax
import jax.numpy as jnp
from jax import lax
from jax.experimental import pallas as pl
from jax.experimental.pallas import tpu as pltpu
from jax.sharding import PartitionSpec as P

MESH = pl.DeviceIdType.MESH
STRIDE = {"x": 16, "y": 8, "h": 4, "l": 2, "c": 1}
DIMS = "xyhl"
ROWS, COLS = 32, 1024
PER_MATRIX = 6
UNITS = 18
KERNEL_VMEM = int(18.25 * 2**20)
GROUP = 3
RING = 3
ORDERS = ("yxhl", "lxyh", "yxlh", "xylh", "lyxh", "xyhl", "yxlh", "lyxh", "xylh", "xyhl", "lyxh", "lxyh", "yxlh", "xyhl", "yxlh", "lxyh", "xylh", "yxlh")
EVENTS = (
    0, 11, 33, 22, 55, 66, 99, 88, 44, 77, 143, 121, 132, 110, 154, 176, 165, 187, 1, 12, 34, 23, 56, 45, 67, 78, 100, 35, 122, 2,
    133, 13, 111, 24, 57, 68, 101, 36, 89, 3, 46, 166, 14, 123, 79, 25, 134, 112, 58, 69, 144, 155, 37, 4, 102, 15, 47, 90, 26,
    80, 167, 135, 124, 70, 59, 188, 5, 177, 38, 103, 136, 16, 48, 145, 60, 156, 27, 81, 91, 6, 104, 113, 39, 168, 71, 61, 17, 189,
    92, 28, 178, 49, 105, 40, 157, 7, 18, 125, 72, 82, 29, 190, 179, 114, 62, 137, 8, 41, 93, 146, 50, 19, 73, 106, 30, 126, 63,
    158, 9, 180, 138, 10, 169, 94, 42, 115, 43, 83, 51, 191, 107, 147, 20, 74, 21, 127, 31, 159, 32, 139, 181, 52, 95, 170, 64,
    65, 116, 84, 148, 192, 160, 75, 182, 76, 128, 108, 109, 53, 96, 54, 140, 149, 171, 117, 85, 193, 161, 183, 129, 150, 141, 142,
    172, 97, 98, 86, 118, 87, 194, 162, 184, 173, 151, 130, 195, 131, 163, 119, 185, 164, 120, 186, 196, 174, 152, 197, 175, 153,
)
TURN = {code // 11: i for i, code in enumerate(c for c in EVENTS if c % 11 == 5)}


def adamw(w, m, v, g):
    m = 0.9 * m + 0.1 * g
    v = 0.95 * v + 0.05 * g * g
    step = m * lax.rsqrt(v + 1e-8) + 0.1 * w
    return (w - 0.02 * step).astype(jnp.bfloat16), m, v


def place(u):
    which, rest = divmod(u, PER_MATRIX)
    layer, part = divmod(rest, PER_MATRIX // 2)
    if which < 2:
        return which, layer, (slice(None), pl.ds(part * COLS, COLS))
    return which, layer, (pl.ds(part * ROWS, ROWS), slice(None))


def blocks(ref, u, at, core):
    _, layer, within = place(u)
    return ref.at[(layer, *(at.get(d, slice(None)) for d in DIMS), core, *within)]


def mine(ref, u):
    _, layer, within = place(u)
    return ref.at[(layer, *within)]


def kernel(*refs):
    g_in, w_in, m_in, v_in = (refs[i : i + 3] for i in range(0, 12, 3))
    n = UNITS // GROUP
    own = [one.at[i] for one in refs[12 : 12 + n] for i in range(GROUP)]
    rx0 = [one.at[i] for one in refs[12 + n : 12 + 2 * n] for i in range(GROUP)]
    g_buf, rx1, rx2, rx3, rx4, w_buf, m_buf, v_buf, rs_send, rs_recv, ag_send, ag_recv, local, free = refs[12 + 2 * n :]
    rx = (rx0, *([one.at[u] for u in range(UNITS)] for one in (rx1, rx2, rx3, rx4)))
    me = lax.axis_index("dp")
    bit = {d: (me // s) % 2 for d, s in STRIDE.items()}
    partner = {d: me + (1 - 2 * bit[d]) * s for d, s in STRIDE.items()}
    every = slice(None)

    barrier = pltpu.get_barrier_semaphore()
    for d in STRIDE:
        pl.semaphore_signal(barrier, inc=1, device_id=(0, partner[d]), device_id_type=MESH)
    pl.semaphore_wait(barrier, len(STRIDE))

    def fixed(u, k, flip):
        at = {d: bit[d] for d in ORDERS[u][:k]}
        if flip:
            at[ORDERS[u][k - 1]] = 1 - bit[ORDERS[u][k - 1]]
        return at

    def remote(src, dst, send, recv, d):
        return pltpu.make_async_remote_copy(
            src_ref=src, dst_ref=dst, send_sem=send, recv_sem=recv, device_id=(0, partner[d]), device_id_type=MESH
        )

    def scatter(u, k):
        if k == 0:
            src, d = blocks(g_in[place(u)[0]], u, {}, 1 - bit["c"]), "c"
        else:
            at, d = fixed(u, k, True), ORDERS[u][k - 1]
            src = own[u].at[tuple(at.get(d, every) for d in DIMS)]
        return remote(src, rx[k][u], rs_send.at[u, k], rs_recv.at[u, k], d)

    def gather(u, k, receive=False):
        if k == 0:
            return remote(own[u], rx0[u], ag_send.at[u, 0], ag_recv.at[u, 0], "c")
        at = fixed(u, k, receive)
        region = own[u].at[tuple(at.get(d, every) for d in DIMS)]
        return remote(region, region, ag_send.at[u, k], ag_recv.at[u, k], ORDERS[u][k - 1])

    def copy(src, dst, u, i):
        return pltpu.make_async_copy(src, dst, local.at[u, i])

    def load_own(u):
        return copy(blocks(g_in[place(u)[0]], u, {}, bit["c"]), own[u], u, 0)

    def loads(u):
        which, slot = place(u)[0], TURN[u] % RING
        return (
            copy(blocks(w_in[which], u, bit, bit["c"]), w_buf.at[slot], u, 1),
            copy(mine(m_in[which], u), m_buf.at[slot], u, 2),
            copy(mine(v_in[which], u), v_buf.at[slot], u, 3),
        )

    def total(u, at, steps, rows):
        so_far = own[u][(*(at[d] for d in DIMS), rows)].astype(jnp.float32)
        for j in range(steps):
            left = [d for d in DIMS if d not in ORDERS[u][:j]]
            so_far += rx[j][u][(*(at[d] for d in left), rows)].astype(jnp.float32)
        return so_far

    def reduce_to_send(u, k):
        base = fixed(u, k, True)
        free = [d for d in DIMS if d not in base]

        def body(i, carry):
            at = dict(base)
            for p, d in enumerate(reversed(free)):
                at[d] = (i // 2**p) % 2
            for half in range(2):
                rows = pl.ds(half * (ROWS // 2), ROWS // 2)
                own[u][(*(at[d] for d in DIMS), rows)] = total(u, at, k, rows).astype(jnp.bfloat16)
            return carry

        lax.fori_loop(0, 2 ** len(free), body, 0)

    def update(u):
        slot = TURN[u] % RING
        for half in range(2):
            rows = pl.ds(half * (ROWS // 2), ROWS // 2)
            g = total(u, bit, 5, rows).astype(jnp.bfloat16)
            g_buf[u, rows] = g
            w, m, v = w_buf[slot, rows].astype(jnp.float32), m_buf[slot, rows], v_buf[slot, rows]
            own[u][(*(bit[d] for d in DIMS), rows)] = adamw(w, m, v, g.astype(jnp.float32))[0]

    def release(u, k):
        pl.semaphore_signal(free.at[u, k], inc=1, device_id=(0, partner[ORDERS[u][k - 1] if k else "c"]), device_id_type=MESH)

    def arrived(u, k):
        scatter(u, k).wait_recv()
        if k:
            scatter(u, k).wait_send()
            release(u, k)

    def send_back(u, k):
        pl.semaphore_wait(free.at[u, k], 1)
        gather(u, k).start()

    def event(u, e):
        if e == 0:
            scatter(u, 0).start()
            load_own(u).start()
        elif e <= 4:
            if e == 1:
                load_own(u).wait()
            arrived(u, e - 1)
            reduce_to_send(u, e)
            scatter(u, e).start()
        elif e == 5:
            for one in loads(u):
                one.wait()
            arrived(u, 4)
            update(u)
            for next_u, turn in TURN.items():
                if turn == TURN[u] + RING:
                    for one in loads(next_u):
                        one.start()
            release(u, 0)
            send_back(u, 4)
        elif e <= 9:
            gather(u, 10 - e, receive=True).wait_recv()
            send_back(u, 9 - e)
        else:
            gather(u, 0, receive=True).wait_recv()

    for u, turn in TURN.items():
        if turn < RING:
            for one in loads(u):
                one.start()
    for code in EVENTS:
        event(*divmod(code, 11))
    for u in range(UNITS):
        scatter(u, 0).wait_send()
        for k in range(5):
            gather(u, k).wait_send()


def write_out(*refs):
    n = UNITS // GROUP
    own, rx0, g_buf = refs[:n], refs[n : 2 * n], refs[2 * n]
    m_in, v_in, w_out, m_out, v_out = (refs[2 * n + i : 2 * n + i + 3] for i in (1, 4, 7, 10, 13))
    m_buf, v_buf, sems = refs[2 * n + 16 :]
    core = lax.axis_index("dp") % 2

    def copy(src, dst, u, i):
        return pltpu.make_async_copy(src, dst, sems.at[u, i])

    def loads(u):
        which = place(u)[0]
        return copy(mine(m_in[which], u), m_buf.at[u], u, 0), copy(mine(v_in[which], u), v_buf.at[u], u, 1)

    def stores(u):
        which = place(u)[0]
        return copy(m_buf.at[u], mine(m_out[which], u), u, 2), copy(v_buf.at[u], mine(v_out[which], u), u, 3)

    def weights(u):
        which = place(u)[0]
        return (
            copy(own[u // GROUP].at[u % GROUP], blocks(w_out[which], u, {}, core), u, 4),
            copy(rx0[u // GROUP].at[u % GROUP], blocks(w_out[which], u, {}, 1 - core), u, 5),
        )

    for u in reversed(range(UNITS)):
        for one in reversed(weights(u)):
            one.start()
    for u in range(UNITS):
        for one in loads(u):
            one.start()
    for u in range(UNITS):
        for one in loads(u):
            one.wait()
        for half in range(2):
            rows = pl.ds(half * (ROWS // 2), ROWS // 2)
            g = g_buf[u, rows].astype(jnp.float32)
            _, m_buf[u, rows], v_buf[u, rows] = adamw(g, m_buf[u, rows], v_buf[u, rows], g)
        for one in stores(u):
            one.start()
    for u in range(UNITS):
        for one in (*weights(u), *stores(u)):
            one.wait()


def solution(mesh):
    def step(*arrays):
        split = [(2, 2, 2, 2, 2, 2, a.shape[-2] // 32, a.shape[-1]) for a in arrays[:3]]
        terms = [a.reshape(s) for a, s in zip(arrays[:3], split)]
        weights = [a.reshape(s) for a, s in zip(arrays[3:6], split)]
        block = (UNITS, ROWS, COLS)
        dma = pltpu.SemaphoreType.DMA
        anywhere = pl.BlockSpec(memory_space=pltpu.HBM)
        vmem = pl.BlockSpec(memory_space=pltpu.VMEM)
        half = pltpu.VMEM((GROUP, 2, 2, 2, 2, ROWS, COLS), jnp.bfloat16)
        kept = pl.pallas_call(
            kernel,
            out_shape=[half] * (2 * UNITS // GROUP) + [pltpu.VMEM(block, jnp.bfloat16)],
            in_specs=[anywhere] * 12,
            out_specs=[vmem] * (2 * UNITS // GROUP + 1),
            scratch_shapes=[
                pltpu.VMEM((UNITS, 2, 2, 2, ROWS, COLS), jnp.bfloat16),
                pltpu.VMEM((UNITS, 2, 2, ROWS, COLS), jnp.bfloat16),
                pltpu.VMEM((UNITS, 2, ROWS, COLS), jnp.bfloat16),
                pltpu.VMEM(block, jnp.bfloat16),
                pltpu.VMEM((RING, ROWS, COLS), jnp.bfloat16),
                pltpu.VMEM((RING, ROWS, COLS), jnp.float32),
                pltpu.VMEM((RING, ROWS, COLS), jnp.float32),
                dma((UNITS, 5)),
                dma((UNITS, 5)),
                dma((UNITS, 5)),
                dma((UNITS, 5)),
                dma((UNITS, 4)),
                pltpu.SemaphoreType.REGULAR((UNITS, 5)),
            ],
            compiler_params=pltpu.CompilerParams(collective_id=0, has_side_effects=True, vmem_limit_bytes=KERNEL_VMEM),
            name="zero_step",
        )(*terms, *weights, *arrays[6:])
        out = pl.pallas_call(
            write_out,
            out_shape=[jax.ShapeDtypeStruct(s, jnp.bfloat16) for s in split] + [jax.ShapeDtypeStruct(a.shape, a.dtype) for a in arrays[6:]],
            in_specs=[vmem] * (2 * UNITS // GROUP + 1) + [anywhere] * 6,
            out_specs=[anywhere] * 9,
            scratch_shapes=[pltpu.VMEM(block, jnp.float32), pltpu.VMEM(block, jnp.float32), dma((UNITS, 6))],
            compiler_params=pltpu.CompilerParams(vmem_limit_bytes=KERNEL_VMEM),
            name="write_out",
        )(*kept, *(pltpu.with_memory_space_constraint(a, pltpu.HBM) for a in arrays[6:]))
        return (*(o.reshape(a.shape) for o, a in zip(out[:3], arrays[3:6])), *out[3:])

    all_of, cut = P(None, None, None), P(None, "dp", None)
    return jax.shard_map(
        step,
        mesh=mesh,
        in_specs=(P(("rep", "dp"), None, None, None),) * 3 + (all_of,) * 3 + (cut,) * 6,
        out_specs=(P("rep", None, None),) * 3 + (P("rep", "dp", None),) * 6,
        check_vma=False,
    )
```

```python
import jax
import jax.numpy as jnp
from jax import lax
from jax.experimental import pallas as pl
from jax.experimental.pallas import tpu as pltpu
from jax.sharding import PartitionSpec as P

MESH = pl.DeviceIdType.MESH
STRIDE = {"x": 16, "y": 8, "h": 4, "l": 2, "c": 1}
DIMS = "xyhl"
ROWS, COLS = 32, 1024
PER_MATRIX = 6
UNITS = 18
KERNEL_VMEM = int(10.75 * 2**20)
GROUP = 6
ORDERS = ("yxhl", "lxyh", "lyxh", "xylh", "xylh", "xylh", "yxlh", "xylh", "lxyh", "lyxh", "lyxh", "yxlh", "xylh", "yxlh", "yxlh", "yxlh", "lxyh", "xylh")
EVENTS = (
    22, 66, 33, 44, 99, 55, 110, 0, 77, 121, 11, 143, 154, 165, 132, 23, 88, 67, 187, 34, 176, 45, 100, 56, 111, 1, 122, 12, 144,
    78, 89, 24, 68, 35, 2, 177, 46, 133, 101, 57, 123, 112, 13, 69, 79, 25, 36, 3, 145, 155, 47, 90, 102, 70, 134, 188, 37, 58,
    124, 166, 48, 4, 71, 26, 113, 59, 38, 80, 178, 125, 146, 14, 5, 49, 72, 91, 27, 156, 103, 81, 60, 39, 135, 147, 6, 126, 50,
    73, 189, 114, 28, 167, 104, 15, 40, 179, 82, 92, 61, 136, 157, 148, 190, 51, 74, 7, 41, 29, 127, 180, 115, 168, 105, 62, 52,
    16, 158, 8, 83, 93, 191, 137, 128, 75, 149, 42, 76, 181, 169, 30, 106, 116, 43, 17, 84, 63, 159, 94, 150, 53, 192, 138, 54, 9,
    129, 117, 10, 170, 107, 18, 31, 182, 160, 32, 85, 139, 64, 193, 95, 171, 65, 151, 19, 108, 130, 161, 109, 131, 194, 118, 172,
    183, 86, 87, 140, 96, 20, 162, 21, 152, 173, 153, 119, 195, 184, 120, 97, 163, 141, 98, 164, 142, 185, 174, 196, 186, 175, 197,
)


def adamw(w, m, v, g):
    m = 0.9 * m + 0.1 * g
    v = 0.95 * v + 0.05 * g * g
    step = m * lax.rsqrt(v + 1e-8) + 0.1 * w
    return (w - 0.02 * step).astype(jnp.bfloat16), m, v


def place(u):
    which, rest = divmod(u, PER_MATRIX)
    layer, part = divmod(rest, PER_MATRIX // 2)
    if which < 2:
        return which, layer, (slice(None), pl.ds(part * COLS, COLS))
    return which, layer, (pl.ds(part * ROWS, ROWS), slice(None))


def blocks(ref, u, at, core):
    _, layer, within = place(u)
    return ref.at[(layer, *(at.get(d, slice(None)) for d in DIMS), core, *within)]


def mine(ref, u):
    _, layer, within = place(u)
    return ref.at[(layer, *within)]


def kernel(*refs):
    g_in, w_in, m_in, v_in = (refs[i : i + 3] for i in range(0, 12, 3))
    n = UNITS // GROUP
    own = [one.at[i] for one in refs[12 : 12 + n] for i in range(GROUP)]
    rx0 = [one.at[i] for one in refs[12 + n : 12 + 2 * n] for i in range(GROUP)]
    m_buf, v_buf, rx1, w_buf, rs_send, rs_recv, ag_send, ag_recv, local, free, ready = refs[12 + 2 * n :]
    me = lax.axis_index("dp")
    bit = {d: (me // s) % 2 for d, s in STRIDE.items()}
    partner = {d: me + (1 - 2 * bit[d]) * s for d, s in STRIDE.items()}
    every = slice(None)

    def later(u, k):
        first = ORDERS[u][0]
        rest = [d for d in DIMS if d != first]
        at = {first: 1 - bit[first], **{d: 1 for d in rest[: k - 2]}, rest[k - 2]: 0}
        return rx0[u].at[tuple(at.get(d, every) for d in DIMS)]

    rx = (rx0, [rx1.at[u] for u in range(UNITS)], *([later(u, k) for u in range(UNITS)] for k in (2, 3, 4)))

    barrier = pltpu.get_barrier_semaphore()
    for d in STRIDE:
        pl.semaphore_signal(barrier, inc=1, device_id=(0, partner[d]), device_id_type=MESH)
    pl.semaphore_wait(barrier, len(STRIDE))

    def fixed(u, k, flip):
        at = {d: bit[d] for d in ORDERS[u][:k]}
        if flip:
            at[ORDERS[u][k - 1]] = 1 - bit[ORDERS[u][k - 1]]
        return at

    def remote(src, dst, send, recv, d):
        return pltpu.make_async_remote_copy(
            src_ref=src, dst_ref=dst, send_sem=send, recv_sem=recv, device_id=(0, partner[d]), device_id_type=MESH
        )

    def scatter(u, k):
        if k == 0:
            src, d = blocks(g_in[place(u)[0]], u, {}, 1 - bit["c"]), "c"
        else:
            at, d = fixed(u, k, True), ORDERS[u][k - 1]
            src = own[u].at[tuple(at.get(d, every) for d in DIMS)]
        return remote(src, rx[k][u], rs_send.at[u, k], rs_recv.at[u, k], d)

    def gather(u, k, receive=False):
        if k == 0:
            return remote(own[u], rx0[u], ag_send.at[u, 0], ag_recv.at[u, 0], "c")
        at = fixed(u, k, receive)
        region = own[u].at[tuple(at.get(d, every) for d in DIMS)]
        return remote(region, region, ag_send.at[u, k], ag_recv.at[u, k], ORDERS[u][k - 1])

    def copy(src, dst, u, i):
        return pltpu.make_async_copy(src, dst, local.at[u, i])

    def load_own(u):
        return copy(blocks(g_in[place(u)[0]], u, {}, bit["c"]), own[u], u, 0)

    def loads(u):
        which = place(u)[0]
        return (
            copy(blocks(w_in[which], u, bit, bit["c"]), w_buf.at[u], u, 1),
            copy(mine(m_in[which], u), m_buf.at[u], u, 2),
            copy(mine(v_in[which], u), v_buf.at[u], u, 3),
        )

    def total(u, at, steps, rows):
        so_far = own[u][(*(at[d] for d in DIMS), rows)].astype(jnp.float32)
        for j in range(steps):
            left = [d for d in DIMS if d not in ORDERS[u][:j]]
            so_far += rx[j][u][(*(at[d] for d in left), rows)].astype(jnp.float32)
        return so_far

    def reduce_to_send(u, k):
        base = fixed(u, k, True)
        free = [d for d in DIMS if d not in base]

        def body(i, carry):
            at = dict(base)
            for p, d in enumerate(reversed(free)):
                at[d] = (i // 2**p) % 2
            for half in range(2):
                rows = pl.ds(half * (ROWS // 2), ROWS // 2)
                own[u][(*(at[d] for d in DIMS), rows)] = total(u, at, k, rows).astype(jnp.bfloat16)
            return carry

        lax.fori_loop(0, 2 ** len(free), body, 0)

    def update(u):
        for half in range(2):
            rows = pl.ds(half * (ROWS // 2), ROWS // 2)
            here = (*(bit[d] for d in DIMS), rows)
            g = total(u, bit, 5, rows).astype(jnp.bfloat16).astype(jnp.float32)
            own[u][here], m_buf[u, rows], v_buf[u, rows] = adamw(w_buf[u, rows].astype(jnp.float32), m_buf[u, rows], v_buf[u, rows], g)

    def release(u, k):
        pl.semaphore_signal(free.at[u, k], inc=1, device_id=(0, partner[ORDERS[u][k - 1] if k else "c"]), device_id_type=MESH)

    def arrived(u, k):
        scatter(u, k).wait_recv()
        if k:
            scatter(u, k).wait_send()
            release(u, k)

    def send_back(u, k):
        pl.semaphore_wait(free.at[u, k], 1)
        gather(u, k).start()

    def event(u, e):
        if e == 0:
            scatter(u, 0).start()
            load_own(u).start()
        elif e <= 4:
            if e == 1:
                load_own(u).wait()
            arrived(u, e - 1)
            reduce_to_send(u, e)
            if e == 1:
                for one in loads(u):
                    one.start()
                for k in (2, 3, 4):
                    pl.semaphore_signal(ready.at[u, k], inc=1, device_id=(0, partner[ORDERS[u][k - 1]]), device_id_type=MESH)
            else:
                pl.semaphore_wait(ready.at[u, e], 1)
            scatter(u, e).start()
        elif e == 5:
            for one in loads(u):
                one.wait()
            arrived(u, 4)
            update(u)
            release(u, 0)
            send_back(u, 4)
        elif e <= 9:
            gather(u, 10 - e, receive=True).wait_recv()
            send_back(u, 9 - e)
        else:
            gather(u, 0, receive=True).wait_recv()

    for code in EVENTS:
        event(*divmod(code, 11))
    for u in range(UNITS):
        scatter(u, 0).wait_send()
        for k in range(5):
            gather(u, k).wait_send()


def write_out(*refs):
    n = UNITS // GROUP
    own, rx0, (m_buf, v_buf) = refs[:n], refs[n : 2 * n], refs[2 * n : 2 * n + 2]
    w_out, m_out, v_out, sems = (*(refs[2 * n + i : 2 * n + i + 3] for i in (2, 5, 8)), refs[2 * n + 11])
    core = lax.axis_index("dp") % 2
    copies = []
    for u in range(UNITS):
        which = place(u)[0]
        for i, (src, dst) in enumerate(
            (
                (own[u // GROUP].at[u % GROUP], blocks(w_out[which], u, {}, core)),
                (rx0[u // GROUP].at[u % GROUP], blocks(w_out[which], u, {}, 1 - core)),
                (m_buf.at[u], mine(m_out[which], u)),
                (v_buf.at[u], mine(v_out[which], u)),
            )
        ):
            copies.append(pltpu.make_async_copy(src, dst, sems.at[u, i]))
    for one in copies:
        one.start()
    for one in copies:
        one.wait()


def solution(mesh):
    def step(*arrays):
        split = [(2, 2, 2, 2, 2, 2, a.shape[-2] // 32, a.shape[-1]) for a in arrays[:3]]
        terms = [a.reshape(s) for a, s in zip(arrays[:3], split)]
        weights = [a.reshape(s) for a, s in zip(arrays[3:6], split)]
        block = (UNITS, ROWS, COLS)
        dma = pltpu.SemaphoreType.DMA
        anywhere = pl.BlockSpec(memory_space=pl.ANY)
        vmem = pl.BlockSpec(memory_space=pltpu.VMEM)
        half = pltpu.VMEM((GROUP, 2, 2, 2, 2, ROWS, COLS), jnp.bfloat16)
        kept = pl.pallas_call(
            kernel,
            out_shape=[half] * (2 * UNITS // GROUP) + [pltpu.VMEM(block, jnp.float32)] * 2,
            in_specs=[anywhere] * 12,
            out_specs=[vmem] * (2 * UNITS // GROUP + 2),
            scratch_shapes=[
                pltpu.VMEM((UNITS, 2, 2, 2, ROWS, COLS), jnp.bfloat16),
                pltpu.VMEM(block, jnp.bfloat16),
                dma((UNITS, 5)),
                dma((UNITS, 5)),
                dma((UNITS, 5)),
                dma((UNITS, 5)),
                dma((UNITS, 4)),
                pltpu.SemaphoreType.REGULAR((UNITS, 5)),
                pltpu.SemaphoreType.REGULAR((UNITS, 5)),
            ],
            compiler_params=pltpu.CompilerParams(collective_id=0, has_side_effects=True, vmem_limit_bytes=KERNEL_VMEM),
            name="zero_step",
        )(*terms, *weights, *(pltpu.with_memory_space_constraint(a, pltpu.HBM) for a in arrays[6:]))
        out = pl.pallas_call(
            write_out,
            out_shape=[jax.ShapeDtypeStruct(s, jnp.bfloat16) for s in split] + [jax.ShapeDtypeStruct(a.shape, a.dtype) for a in arrays[6:]],
            in_specs=[vmem] * (2 * UNITS // GROUP + 2),
            out_specs=[anywhere] * 9,
            scratch_shapes=[dma((UNITS, 4))],
            compiler_params=pltpu.CompilerParams(vmem_limit_bytes=KERNEL_VMEM),
            name="write_out",
        )(*kept)
        return (*(o.reshape(a.shape) for o, a in zip(out[:3], arrays[3:6])), *out[3:])

    all_of, cut = P(None, None, None), P(None, "dp", None)
    return jax.shard_map(
        step,
        mesh=mesh,
        in_specs=(P(("rep", "dp"), None, None, None),) * 3 + (all_of,) * 3 + (cut,) * 6,
        out_specs=(P("rep", None, None),) * 3 + (P("rep", "dp", None),) * 6,
        check_vma=False,
    )
```
